32 devices in a mesh: dp: 4 (over z), expert: 8 (over y, x, core).
Axes of the slice: x: 2, y: 2, z: 4, core: 2. Of those that a mesh axis runs over, the one named last changes fastest.
Arguments:
- tokens: bfloat16 [256, 192, 1024], P(None, ('dp', 'expert')), may hold values from -200 to 200
- grad_out: bfloat16 [256, 192, 1024], P(None, ('dp', 'expert')), may hold values from -6 to 6
- slot_out: bfloat16 [512, 192, 1024], P('expert', 'dp'), may hold values from -6 to 6
- slot_params: bfloat16 [512, 1024], P('expert'), may hold values from -2 to 2
Outputs:
- grad_tokens: bfloat16 [256, 192, 1024], P(None, ('dp', 'expert'))
- grad_slot_out: bfloat16 [512, 192, 1024], P('expert', 'dp')
- grad_params: float32 [512, 1024], P('expert', 'dp')
The draws below stay inside these ranges and needn't reach their ends.
All inputs are finite; a program needn't handle non-finite values.
Results may differ from the reference program's by a relative error of at most 0.018.
Values may be sent and summed in bfloat16 or wider, within the bound.
A program may use at most 128 MiB of HBM per device.

```python
import math
import jax
import jax.numpy as jnp

D = 1024
SLOTS = 512
PATCHES = 256
IMAGES = 192


def slot_table(key):
    inner = jax.random.fold_in(key, 11)
    spread = 2.0 / math.sqrt(D)
    values = jnp.clip(jax.random.normal(inner, (SLOTS, D)) * spread, -6.0 * spread, 6.0 * spread)
    return values.astype(jnp.bfloat16).astype(jnp.float32)


def draw_slot_params(key, part):
    return slot_table(key).astype(jnp.bfloat16)


def draw_tokens(key, part):
    key_base = jax.random.fold_in(jax.random.fold_in(key, 23), 0)
    values = jnp.clip(jax.random.normal(key_base, (PATCHES, IMAGES, D)), -6.0, 6.0)
    return values.astype(jnp.bfloat16)


def block_levels(own_key, dims, pieces, smallest, largest):
    level, own = 1.0, jax.random.fold_in(own_key, 6)
    for axis_at, parts in pieces:
        steps = jnp.exp(jax.random.uniform(jax.random.fold_in(own, axis_at), (parts,), jnp.float32, smallest / len(pieces), largest / len(pieces)))
        level = level * jnp.repeat(steps, dims[axis_at] // parts).reshape([-1 if axis == axis_at else 1 for axis in range(len(dims))])
    return level


def gaussian(rng, dims, width, reach, cuts=(), kind=jnp.bfloat16):
    loudness = block_levels(rng, dims, cuts, -0.22, 0.18) if cuts else 1.0
    drawn = jax.random.normal(rng, dims, jnp.float32) * width * loudness
    return jnp.minimum(jnp.maximum(drawn, -reach), reach).astype(kind)


def setup_inputs(seed: int = 0) -> dict:
    key_of = jax.random.split(jax.random.key(seed), 5)
    return {
        "tokens": draw_tokens(jax.random.fold_in(key_of[4], 71), 0),
        "grad_out": gaussian(key_of[1], (PATCHES, IMAGES, D), 1.0, 6.0, ((1, 32),)),
        "slot_out": gaussian(key_of[2], (SLOTS, IMAGES, D), 1.0, 6.0, ((0, 8), (1, 4))),
        "slot_params": draw_slot_params(jax.random.fold_in(key_of[4], 71), 0),
    }


def reference(tokens, grad_out, slot_out, slot_params):
    tok_wide = tokens.astype(jnp.float32)
    grad_wide = grad_out.astype(jnp.float32)
    param_wide = slot_params.astype(jnp.float32)
    logits = jnp.einsum('tbd,sd->tbs', tok_wide, param_wide)
    combine = jax.nn.softmax(logits, axis=-1)
    combine_low = combine.astype(jnp.bfloat16)
    grad_slot = jnp.einsum('tbs,tbd->sbd', combine_low.astype(jnp.float32), grad_wide).astype(jnp.bfloat16)
    grad_comb = jnp.einsum('tbd,sbd->tbs', grad_wide, slot_out.astype(jnp.float32))
    rowdot = jnp.sum(combine * grad_comb, axis=-1, keepdims=True)
    grad_logits = (combine * (grad_comb - rowdot)).astype(jnp.bfloat16)
    logit_wide = grad_logits.astype(jnp.float32)
    grad_tok = jnp.einsum('tbs,sd->tbd', logit_wide, param_wide).astype(jnp.bfloat16)
    grad_params = jnp.einsum('tbs,tbd->sd', logit_wide, tok_wide)
    return grad_tok, grad_slot, grad_params
```

```python
import functools

import jax
import jax.numpy as jnp
from jax import lax
from jax.experimental import pallas as pl
from jax.experimental.pallas import tpu as pltpu
from jax.sharding import PartitionSpec as P

BF = jnp.bfloat16
F32 = jnp.float32
GROUP = 16


def flip(index, mask, size):
    total, bit = 0, 1
    while bit < size:
        total = total + ((index // bit + mask // bit) % 2) * bit
        bit *= 2
    return total


def send_order(n, core):
    if n != 8:
        return list(range(n - 1, 0, -1))
    masks = []
    for low in range(2):
        masks += [6 + low - 4 * core, 2 + low + 2 * core, 4 + low + 2 * core]
    return masks + [1]


def rows_last(lhs, rhs):
    return lax.dot_general(lhs, rhs, (((1,), (1,)), ((), ())), preferred_element_type=F32)


def exchange_kernel(
    n, m, tok_hbm, go_hbm, so_hbm, par_hbm,
    grec, gt_out, gp_out,
    tok, go, so, par, allp, stage, rows, gs, comb, gt, acc, psend, precv, xsend, xrecv, gp,
    local_sem, p_send, p_recv, q_send, q_recv, a_send, a_recv, g_send, g_recv,
    z_send, z_recv, x_send, x_recv,
):
    me = lax.axis_index("expert")
    mz = lax.axis_index("dp")
    core = me % 2
    imgs = tok.shape[0]
    own = par.shape[0]
    all_img = so.shape[1]
    cols = allp.shape[1] // m
    width = allp.shape[1]
    slots = allp.shape[0]
    my_cols = pl.ds(pl.multiple_of(mz * cols, 128), cols)
    my_rows = pl.ds(pl.multiple_of(me * own, GROUP), own)

    loads = [
        pltpu.make_async_copy(src, dst, local_sem.at[i])
        for i, (src, dst) in enumerate([(par_hbm, par), (so_hbm, so), (tok_hbm, tok), (go_hbm, go)])
    ]
    for load in loads:
        load.start()

    barrier = pltpu.get_barrier_semaphore()
    for k in range(1, n):
        pl.semaphore_signal(barrier, inc=1, device_id=(mz, flip(me, k, n)), device_id_type=pl.DeviceIdType.MESH)
    for k in range(1, m):
        pl.semaphore_signal(barrier, inc=1, device_id=(flip(mz, k, m), me), device_id_type=pl.DeviceIdType.MESH)
    pl.semaphore_wait(barrier, n + m - 2)

    def to_expert(src, dst, send, recv, k):
        return pltpu.make_async_remote_copy(
            src_ref=src, dst_ref=dst, send_sem=send.at[k], recv_sem=recv.at[k],
            device_id=(mz, flip(me, k, n)), device_id_type=pl.DeviceIdType.MESH,
        )

    def to_dp(src, dst, send, recv, k):
        return pltpu.make_async_remote_copy(
            src_ref=src, dst_ref=dst, send_sem=send.at[k], recv_sem=recv.at[k],
            device_id=(flip(mz, k, m), me), device_id_type=pl.DeviceIdType.MESH,
        )

    loads[0].wait()
    p_copies = [to_expert(par.at[:, my_cols], allp.at[my_rows, my_cols], p_send, p_recv, k) for k in range(1, n)]
    for copy in p_copies:
        copy.start()
    allp[my_rows, my_cols] = par[:, my_cols]

    loads[1].wait()
    out_r = lax.broadcasted_iota(jnp.int32, (imgs * GROUP, GROUP * all_img), 0)
    in_c = lax.broadcasted_iota(jnp.int32, (imgs * GROUP, GROUP * all_img), 1)
    base = in_c - (out_r % GROUP) * all_img - out_r // GROUP

    def relayout(dest, out):
        pick = jnp.where(base == dest * imgs, 1.0, 0.0).astype(BF)

        def one(g, carry):
            s0 = pl.multiple_of(g * GROUP, GROUP)
            block = so[pl.ds(s0, GROUP)].reshape(GROUP * all_img, width)
            moved = jnp.dot(pick, block, preferred_element_type=F32).astype(BF)
            out[:, pl.ds(s0, GROUP), :] = moved.reshape(imgs, GROUP, width)
            return carry

        lax.fori_loop(0, own // GROUP, one, 0)

    order = send_order(n, core)
    a_copies = []
    for k in order:
        relayout(flip(me, k, n), stage.at[k])
        copy = to_expert(stage.at[k], rows.at[me], a_send, a_recv, k)
        copy.start()
        a_copies.append(copy)
    relayout(me, rows.at[me])

    for copy in p_copies:
        copy.wait_recv()
    q_copies = [to_dp(allp.at[:, my_cols], allp.at[:, my_cols], q_send, q_recv, k) for k in range(1, m)]
    for copy in q_copies:
        copy.start()
    loads[2].wait()
    loads[3].wait()
    for copy in q_copies:
        copy.wait_recv()

    def forward(b, carry):
        logits = rows_last(allp[...], tok[b])
        peak = jnp.max(logits, axis=0, keepdims=True)
        raised = jnp.exp(logits - peak)
        weights = raised / jnp.sum(raised, axis=0, keepdims=True)
        comb[b] = weights
        grads = jnp.dot(weights.astype(BF), go[b], preferred_element_type=F32).astype(BF)
        gs[:, b] = grads.reshape(n, own, width)
        return carry

    lax.fori_loop(0, imgs, forward, 0)

    keep = pltpu.make_async_copy(gs.at[me], grec.at[me], local_sem.at[4])
    keep.start()
    g_copies = []
    for k in order:
        copy = to_expert(gs.at[flip(me, k, n)], grec.at[me], g_send, g_recv, k)
        copy.start()
        g_copies.append(copy)

    for copy in a_copies:
        copy.wait_recv()
    acc[...] = jnp.zeros_like(acc)

    def backward(b, carry):
        grad_comb = rows_last(rows[:, b].reshape(slots, width), go[b])
        weights = comb[b]
        rowdot = jnp.sum(weights * grad_comb, axis=0, keepdims=True)
        wide = weights * (grad_comb - rowdot)
        acc[...] += jnp.dot(wide.astype(BF), tok[b], preferred_element_type=F32)
        gt[b] = jnp.dot(wide.T.astype(BF), allp[...], preferred_element_type=F32).astype(BF)
        return carry

    lax.fori_loop(0, imgs, backward, 0)

    for k in range(1, m):
        there = flip(mz, k, m)
        psend[k] = acc[:, pl.ds(pl.multiple_of(there * cols, 128), cols)].astype(BF)
    z_copies = [to_dp(psend.at[k], precv.at[k], z_send, z_recv, k) for k in range(1, m)]
    for copy in z_copies:
        copy.start()
    put = pltpu.make_async_copy(gt, gt_out, local_sem.at[5])
    put.start()
    for copy in z_copies:
        copy.wait_recv()
    total = acc[:, my_cols]
    for k in range(1, m):
        total = total + precv[k].astype(F32)
    acc[:, my_cols] = total
    for k in range(1, n):
        there = flip(me, k, n)
        xsend[k] = acc[pl.ds(pl.multiple_of(there * own, GROUP), own), my_cols].astype(BF)
    x_copies = [to_expert(xsend.at[k], xrecv.at[k], x_send, x_recv, k) for k in range(1, n)]
    for copy in x_copies:
        copy.start()
    for copy in x_copies:
        copy.wait_recv()
    owned = acc[my_rows, my_cols]
    for k in range(1, n):
        owned = owned + xrecv[k].astype(F32)
    gp[...] = owned
    give = pltpu.make_async_copy(gp, gp_out, local_sem.at[6])
    give.start()

    for copy in g_copies:
        copy.wait_recv()
    for copy in p_copies + a_copies + q_copies + g_copies + z_copies + x_copies:
        copy.wait_send()
    keep.wait()
    put.wait()
    give.wait()


def exchange(n, m, tok, go, so, par):
    imgs, patches, width = tok.shape
    own, all_img, _ = so.shape
    slots, cols = own * n, width // m
    dma = pltpu.SemaphoreType.DMA
    return pl.pallas_call(
        functools.partial(exchange_kernel, n, m),
        out_shape=(
            jax.ShapeDtypeStruct((n, imgs, own, width), BF),
            jax.ShapeDtypeStruct((imgs, patches, width), BF),
            jax.ShapeDtypeStruct((own, cols), F32),
        ),
        in_specs=[pl.BlockSpec(memory_space=pl.ANY)] * 4,
        out_specs=(pl.BlockSpec(memory_space=pl.ANY),) * 3,
        scratch_shapes=[
            pltpu.VMEM((imgs, patches, width), BF),
            pltpu.VMEM((imgs, patches, width), BF),
            pltpu.VMEM((own, all_img, width), BF),
            pltpu.VMEM((own, width), BF),
            pltpu.VMEM((slots, width), BF),
            pltpu.VMEM((n, imgs, own, width), BF),
            pltpu.VMEM((n, imgs, own, width), BF),
            pltpu.VMEM((n, imgs, own, width), BF),
            pltpu.VMEM((imgs, slots, patches), F32),
            pltpu.VMEM((imgs, patches, width), BF),
            pltpu.VMEM((slots, width), F32),
            pltpu.VMEM((m, slots, cols), BF),
            pltpu.VMEM((m, slots, cols), BF),
            pltpu.VMEM((n, own, cols), BF),
            pltpu.VMEM((n, own, cols), BF),
            pltpu.VMEM((own, cols), F32),
            dma((7,)),
            dma((n,)), dma((n,)), dma((m,)), dma((m,)),
            dma((n,)), dma((n,)), dma((n,)), dma((n,)),
            dma((m,)), dma((m,)), dma((n,)), dma((n,)),
        ],
        compiler_params=pltpu.CompilerParams(
            collective_id=0, has_side_effects=True, vmem_limit_bytes=66 * 1000 * 1000
        ),
    )(tok, go, so, par)


def settle_kernel(arrived, gp_in, out, gp_out):
    all_img, group, width = arrived.shape
    span = GROUP * group
    row = lax.broadcasted_iota(jnp.int32, (span, span), 0)
    col = lax.broadcasted_iota(jnp.int32, (span, span), 1)
    pick = jnp.where(col == (row % GROUP) * group + row // GROUP, 1.0, 0.0).astype(BF)
    for at in range(0, all_img, GROUP):
        block = arrived[at : at + GROUP].reshape(span, width)
        moved = jnp.dot(pick, block, preferred_element_type=F32).astype(BF)
        out[:, at : at + GROUP, :] = moved.reshape(group, GROUP, width)
    gp_out[...] = gp_in[...]


def settle(arrived, grad_par):
    all_img, own, width = arrived.shape
    small = pl.BlockSpec((GROUP, grad_par.shape[1]), lambda i: (i, 0))
    return pl.pallas_call(
        settle_kernel,
        grid=(own // GROUP,),
        out_shape=(
            jax.ShapeDtypeStruct((own, all_img, width), BF),
            jax.ShapeDtypeStruct(grad_par.shape, F32),
        ),
        in_specs=[pl.BlockSpec((all_img, GROUP, width), lambda i: (0, i, 0)), small],
        out_specs=(pl.BlockSpec((GROUP, all_img, width), lambda i: (i, 0, 0)), small),
    )(arrived, grad_par)


def per_device(n, m, tokens, grad_out, slot_out, slot_params):
    tok = jnp.transpose(tokens, (1, 0, 2))
    go = jnp.transpose(grad_out, (1, 0, 2))
    arrived, grad_tok, grad_par = exchange(n, m, tok, go, slot_out, slot_params)
    own, all_img, width = slot_out.shape
    grad_slot, grad_par = settle(arrived.reshape(all_img, own, width), grad_par)
    return jnp.transpose(grad_tok, (1, 0, 2)), grad_slot, grad_par


def solution(mesh):
    return jax.shard_map(
        functools.partial(per_device, mesh.shape["expert"], mesh.shape["dp"]),
        mesh=mesh,
        in_specs=(
            P(None, ("dp", "expert"), None),
            P(None, ("dp", "expert"), None),
            P("expert", "dp", None),
            P("expert", None),
        ),
        out_specs=(P(None, ("dp", "expert"), None), P("expert", "dp", None), P("expert", "dp")),
        check_vma=False,
    )
```

```python
import functools

import jax
import jax.numpy as jnp
from jax import lax
from jax.experimental import pallas as pl
from jax.experimental.pallas import tpu as pltpu
from jax.sharding import PartitionSpec as P

BF = jnp.bfloat16
F32 = jnp.float32
GROUP = 16


def flip(index, mask, size):
    total, bit = 0, 1
    while bit < size:
        total = total + ((index // bit + mask // bit) % 2) * bit
        bit *= 2
    return total


def send_order(n, core):
    if n != 8:
        return list(range(n - 1, 0, -1))
    masks = []
    for low in range(2):
        masks += [6 + low - 4 * core, 2 + low + 2 * core, 4 + low + 2 * core]
    return masks + [1]


def rows_last(lhs, rhs):
    return lax.dot_general(lhs, rhs, (((1,), (1,)), ((), ())), preferred_element_type=F32)


def exchange_kernel(
    n, m, tok_hbm, go_hbm, so_hbm, par_hbm,
    grec, gt_out, gp_out,
    tok, go, so, par, allp, stage, rows, gs, comb, gt, acc, psend, precv, xsend, xrecv, gp,
    local_sem, p_send, p_recv, q_send, q_recv, a_send, a_recv, g_send, g_recv,
    z_send, z_recv, x_send, x_recv,
):
    me = lax.axis_index("expert")
    mz = lax.axis_index("dp")
    core = me % 2
    imgs = tok.shape[0]
    own = par.shape[0]
    all_img = so.shape[1]
    cols = allp.shape[1] // m
    width = allp.shape[1]
    slots = allp.shape[0]
    my_cols = pl.ds(pl.multiple_of(mz * cols, 128), cols)
    my_rows = pl.ds(pl.multiple_of(me * own, GROUP), own)

    loads = [
        pltpu.make_async_copy(src, dst, local_sem.at[i])
        for i, (src, dst) in enumerate([(par_hbm, par), (so_hbm, so), (tok_hbm, tok), (go_hbm, go)])
    ]
    for load in loads:
        load.start()

    barrier = pltpu.get_barrier_semaphore()
    for k in range(1, n):
        pl.semaphore_signal(barrier, inc=1, device_id=(mz, flip(me, k, n)), device_id_type=pl.DeviceIdType.MESH)
    for k in range(1, m):
        pl.semaphore_signal(barrier, inc=1, device_id=(flip(mz, k, m), me), device_id_type=pl.DeviceIdType.MESH)
    pl.semaphore_wait(barrier, n + m - 2)

    def to_expert(src, dst, send, recv, k):
        return pltpu.make_async_remote_copy(
            src_ref=src, dst_ref=dst, send_sem=send.at[k], recv_sem=recv.at[k],
            device_id=(mz, flip(me, k, n)), device_id_type=pl.DeviceIdType.MESH,
        )

    def to_dp(src, dst, send, recv, k):
        return pltpu.make_async_remote_copy(
            src_ref=src, dst_ref=dst, send_sem=send.at[k], recv_sem=recv.at[k],
            device_id=(flip(mz, k, m), me), device_id_type=pl.DeviceIdType.MESH,
        )

    loads[0].wait()
    p_copies = [to_expert(par.at[:, my_cols], allp.at[my_rows, my_cols], p_send, p_recv, k) for k in range(1, n)]
    for copy in p_copies:
        copy.start()
    allp[my_rows, my_cols] = par[:, my_cols]

    loads[1].wait()
    out_r = lax.broadcasted_iota(jnp.int32, (imgs * GROUP, GROUP * all_img), 0)
    in_c = lax.broadcasted_iota(jnp.int32, (imgs * GROUP, GROUP * all_img), 1)
    base = in_c - (out_r % GROUP) * all_img - out_r // GROUP

    def relayout(dest, out):
        pick = jnp.where(base == dest * imgs, 1.0, 0.0).astype(BF)

        def one(g, carry):
            s0 = pl.multiple_of(g * GROUP, GROUP)
            block = so[pl.ds(s0, GROUP)].reshape(GROUP * all_img, width)
            moved = jnp.dot(pick, block, preferred_element_type=F32).astype(BF)
            out[:, pl.ds(s0, GROUP), :] = moved.reshape(imgs, GROUP, width)
            return carry

        lax.fori_loop(0, own // GROUP, one, 0)

    order = send_order(n, core)
    a_copies = []
    for k in order:
        relayout(flip(me, k, n), stage.at[k])
        copy = to_expert(stage.at[k], rows.at[me], a_send, a_recv, k)
        copy.start()
        a_copies.append(copy)
    relayout(me, rows.at[me])

    for copy in p_copies:
        copy.wait_recv()
    q_copies = [to_dp(allp.at[:, my_cols], allp.at[:, my_cols], q_send, q_recv, k) for k in range(1, m)]
    for copy in q_copies:
        copy.start()
    loads[2].wait()
    loads[3].wait()
    for copy in q_copies:
        copy.wait_recv()

    def forward(b, carry):
        logits = rows_last(allp[...], tok[b])
        peak = jnp.max(logits, axis=0, keepdims=True)
        raised = jnp.exp(logits - peak)
        weights = raised / jnp.sum(raised, axis=0, keepdims=True)
        comb[b] = weights
        grads = jnp.dot(weights.astype(BF), go[b], preferred_element_type=F32).astype(BF)
        gs[:, b] = grads.reshape(n, own, width)
        return carry

    lax.fori_loop(0, imgs, forward, 0)

    keep = pltpu.make_async_copy(gs.at[me], grec.at[me], local_sem.at[4])
    keep.start()
    g_copies = []
    for k in order:
        copy = to_expert(gs.at[flip(me, k, n)], grec.at[me], g_send, g_recv, k)
        copy.start()
        g_copies.append(copy)

    for copy in a_copies:
        copy.wait_recv()
    acc[...] = jnp.zeros_like(acc)

    def backward(b, carry):
        grad_comb = rows_last(rows[:, b].reshape(slots, width), go[b])
        weights = comb[b]
        rowdot = jnp.sum(weights * grad_comb, axis=0, keepdims=True)
        wide = weights * (grad_comb - rowdot)
        acc[...] += jnp.dot(wide.astype(BF), tok[b], preferred_element_type=F32)
        gt[b] = jnp.dot(wide.T.astype(BF), allp[...], preferred_element_type=F32).astype(BF)
        return carry

    lax.fori_loop(0, imgs, backward, 0)

    for k in range(1, m):
        there = flip(mz, k, m)
        psend[k] = acc[:, pl.ds(pl.multiple_of(there * cols, 128), cols)].astype(BF)
    z_copies = [to_dp(psend.at[k], precv.at[k], z_send, z_recv, k) for k in range(1, m)]
    for copy in z_copies:
        copy.start()
    put = pltpu.make_async_copy(gt, gt_out, local_sem.at[5])
    put.start()
    for copy in z_copies:
        copy.wait_recv()
    total = acc[:, my_cols]
    for k in range(1, m):
        total = total + precv[k].astype(F32)
    acc[:, my_cols] = total
    for k in range(1, n):
        there = flip(me, k, n)
        xsend[k] = acc[pl.ds(pl.multiple_of(there * own, GROUP), own), my_cols].astype(BF)
    x_copies = [to_expert(xsend.at[k], xrecv.at[k], x_send, x_recv, k) for k in range(1, n)]
    for copy in x_copies:
        copy.start()
    for copy in x_copies:
        copy.wait_recv()
    owned = acc[my_rows, my_cols]
    for k in range(1, n):
        owned = owned + xrecv[k].astype(F32)
    gp[...] = owned
    give = pltpu.make_async_copy(gp, gp_out, local_sem.at[6])
    give.start()

    for copy in g_copies:
        copy.wait_recv()
    for copy in p_copies + a_copies + q_copies + g_copies + z_copies + x_copies:
        copy.wait_send()
    keep.wait()
    put.wait()
    give.wait()


def exchange(n, m, tok, go, so, par):
    imgs, patches, width = tok.shape
    own, all_img, _ = so.shape
    slots, cols = own * n, width // m
    dma = pltpu.SemaphoreType.DMA
    return pl.pallas_call(
        functools.partial(exchange_kernel, n, m),
        out_shape=(
            jax.ShapeDtypeStruct((n, imgs, own, width), BF),
            jax.ShapeDtypeStruct((imgs, patches, width), BF),
            jax.ShapeDtypeStruct((own, cols), F32),
        ),
        in_specs=[pl.BlockSpec(memory_space=pl.ANY)] * 4,
        out_specs=(pl.BlockSpec(memory_space=pl.ANY),) * 3,
        scratch_shapes=[
            pltpu.VMEM((imgs, patches, width), BF),
            pltpu.VMEM((imgs, patches, width), BF),
            pltpu.VMEM((own, all_img, width), BF),
            pltpu.VMEM((own, width), BF),
            pltpu.VMEM((slots, width), BF),
            pltpu.VMEM((n, imgs, own, width), BF),
            pltpu.VMEM((n, imgs, own, width), BF),
            pltpu.VMEM((n, imgs, own, width), BF),
            pltpu.VMEM((imgs, slots, patches), F32),
            pltpu.VMEM((imgs, patches, width), BF),
            pltpu.VMEM((slots, width), F32),
            pltpu.VMEM((m, slots, cols), BF),
            pltpu.VMEM((m, slots, cols), BF),
            pltpu.VMEM((n, own, cols), BF),
            pltpu.VMEM((n, own, cols), BF),
            pltpu.VMEM((own, cols), F32),
            dma((7,)),
            dma((n,)), dma((n,)), dma((m,)), dma((m,)),
            dma((n,)), dma((n,)), dma((n,)), dma((n,)),
            dma((m,)), dma((m,)), dma((n,)), dma((n,)),
        ],
        compiler_params=pltpu.CompilerParams(
            collective_id=0, has_side_effects=True, vmem_limit_bytes=66 * 1000 * 1000
        ),
    )(tok, go, so, par)


AXES = ((2, (4, 5, 1)), (4, (2, 3, 1)))


def side_spot(which, index):
    high = index // 4 if which == 0 else (index // 2) % 2
    return high * 2 + index % 2


def paired_kernel(
    n, m, tok_hbm, go_hbm, so_hbm, par_hbm,
    grec, gt_out, gp_out,
    tok, go, mate, so, par, allp, stage, rows, gs, comb, gcf, low, low_send, gc_send, gc_recv,
    gt, acc, psend, precv, xsend, xrecv, gp,
    local_sem, keep_sem, p_send, p_recv, q_send, q_recv, o_send, o_recv, a_send, a_recv, w_send, w_recv,
    c_send, c_recv, g_send, g_recv, z_send, z_recv, x_send, x_recv,
):
    me = lax.axis_index("expert")
    mz = lax.axis_index("dp")
    imgs = tok.shape[0]
    half = imgs // 2
    own = par.shape[0]
    all_img = so.shape[1]
    slots, width = allp.shape
    patches = tok.shape[1]
    cols = width // m
    quarter = slots // 4
    my_cols = pl.ds(pl.multiple_of(mz * cols, 128), cols)
    my_rows = pl.ds(pl.multiple_of(me * own, GROUP), own)
    sides = ((me // 2) % 2, me // 4)

    def piece(which, other, p):
        side = 1 - sides[which] if other else sides[which]
        start = p * 2 * quarter + side * quarter if which == 0 else side * 2 * quarter + p * quarter
        return pl.ds(pl.multiple_of(start, quarter), quarter)

    loads = [
        pltpu.make_async_copy(src, dst, local_sem.at[i])
        for i, (src, dst) in enumerate([(par_hbm, par), (so_hbm, so), (tok_hbm, tok), (go_hbm, go)])
    ]
    for i in (0, 3, 1, 2):
        loads[i].start()

    barrier = pltpu.get_barrier_semaphore()
    for k in range(1, n):
        pl.semaphore_signal(barrier, inc=1, device_id=(mz, flip(me, k, n)), device_id_type=pl.DeviceIdType.MESH)
    for k in range(1, m):
        pl.semaphore_signal(barrier, inc=1, device_id=(flip(mz, k, m), me), device_id_type=pl.DeviceIdType.MESH)
    pl.semaphore_wait(barrier, n + m - 2)

    def to_expert(src, dst, send, recv, k):
        return pltpu.make_async_remote_copy(
            src_ref=src, dst_ref=dst, send_sem=send, recv_sem=recv,
            device_id=(mz, flip(me, k, n)), device_id_type=pl.DeviceIdType.MESH,
        )

    def to_dp(src, dst, send, recv):
        return [
            pltpu.make_async_remote_copy(
                src_ref=src(k), dst_ref=dst(k), send_sem=send.at[k], recv_sem=recv.at[k],
                device_id=(flip(mz, k, m), me), device_id_type=pl.DeviceIdType.MESH,
            )
            for k in range(1, m)
        ]

    sent = []

    def launch(copies):
        for copy in copies:
            copy.start()
        sent.extend(copies)
        return copies

    def arrive(copies):
        for copy in copies:
            copy.wait_recv()

    loads[0].wait()
    p_copies = launch([
        to_expert(par.at[:, my_cols], allp.at[my_rows, my_cols], p_send.at[k], p_recv.at[k], k) for k in range(1, n)
    ])
    allp[my_rows, my_cols] = par[:, my_cols]
    loads[3].wait()
    o_copies = launch([
        to_expert(go.at[pl.ds(q * half, half)], mate.at[q], o_send.at[q], o_recv.at[q], AXES[q][0]) for q in range(2)
    ])

    loads[1].wait()
    out_r = lax.broadcasted_iota(jnp.int32, (imgs * GROUP, GROUP * all_img), 0)
    in_c = lax.broadcasted_iota(jnp.int32, (imgs * GROUP, GROUP * all_img), 1)
    base = in_c - (out_r % GROUP) * all_img - (out_r // GROUP) % half
    first = out_r < half * GROUP

    def relayout(q, dest, out):
        own_at = dest * imgs + q * half
        mate_at = flip(dest, AXES[q][0], n) * imgs + q * half
        pick = jnp.where(base == jnp.where(first, own_at, mate_at), 1.0, 0.0).astype(BF)

        def one(g, carry):
            s0 = pl.multiple_of(g * GROUP, GROUP)
            block = so[pl.ds(s0, GROUP)].reshape(GROUP * all_img, width)
            moved = jnp.dot(pick, block, preferred_element_type=F32).astype(BF)
            out[:, pl.ds(s0, GROUP), :] = moved.reshape(imgs, GROUP, width)
            return carry

        lax.fori_loop(0, own // GROUP, one, 0)

    a_copies = []
    for i in range(3):
        for q in range(2):
            k = AXES[q][1][i]
            relayout(q, flip(me, k, n), stage.at[q, i])
            a_copies += launch([
                to_expert(stage.at[q, i], rows.at[q, side_spot(q, me)], a_send.at[q, i], a_recv.at[q, i], k)
            ])
    for q in range(2):
        relayout(q, me, rows.at[q, side_spot(q, me)])

    arrive(p_copies)
    q_copies = launch(to_dp(lambda k: allp.at[:, my_cols], lambda k: allp.at[:, my_cols], q_send, q_recv))
    loads[2].wait()
    arrive(q_copies)

    w_copies = []
    for q in range(2):

        def forward(t, carry):
            b = q * half + t
            logits = rows_last(allp[...], tok[b])
            peak = jnp.max(logits, axis=0, keepdims=True)
            raised = jnp.exp(logits - peak)
            comb[b] = raised / jnp.sum(raised, axis=0, keepdims=True)
            for p in range(2):
                low[q, t, p * quarter : (p + 1) * quarter] = comb[b, piece(q, False, p)].astype(BF)
                low_send[q, t, p * quarter : (p + 1) * quarter] = comb[b, piece(q, True, p)].astype(BF)
            return carry

        lax.fori_loop(0, half, forward, 0)
        w_copies += launch([
            to_expert(low_send.at[q], low.at[q, pl.ds(half, half)], w_send.at[q], w_recv.at[q], AXES[q][0])
        ])

    def slot_grads(q, i, grads_in):
        out = jnp.dot(low[q, i], grads_in, preferred_element_type=F32).astype(BF)
        gs[q, :, i] = out.reshape(4, own, width)

    def comb_grads(q, i, grads_in):
        return rows_last(rows[q, :, i].reshape(4 * own, width), grads_in)

    for q in range(2):

        def own_slots(t, carry):
            slot_grads(q, t, go[q * half + t])
            return carry

        lax.fori_loop(0, half, own_slots, 0)

    arrive(o_copies)
    arrive(a_copies)
    c_copies = []
    for q in range(2):

        def mate_comb(t, carry):
            gc_send[q, t] = comb_grads(q, half + t, mate[q, t]).astype(BF)
            return carry

        lax.fori_loop(0, half, mate_comb, 0)
        c_copies += launch([to_expert(gc_send.at[q], gc_recv.at[q], c_send.at[q], c_recv.at[q], AXES[q][0])])

    keeps = []

    def return_grads(h):
        copies = []
        for i in range(3):
            for q in range(2):
                k = AXES[q][1][i]
                holder = flip(me, AXES[q][0], n) if h else me
                part, images = pl.ds(h * half, half), pl.ds(q * half, half)
                copies += launch([
                    to_expert(
                        gs.at[q, side_spot(q, flip(me, k, n)), part], grec.at[holder, images],
                        g_send.at[h, q, i], g_recv.at[h, q, i], k,
                    )
                ])
        for q in range(2):
            holder = flip(me, AXES[q][0], n) if h else me
            keep = pltpu.make_async_copy(
                gs.at[q, side_spot(q, me), pl.ds(h * half, half)],
                grec.at[holder, pl.ds(q * half, half)], keep_sem.at[h, q],
            )
            keep.start()
            keeps.append(keep)
        return copies

    g_copies = return_grads(0)
    arrive(w_copies)
    for q in range(2):

        def mate_slots(t, carry):
            slot_grads(q, half + t, mate[q, t])
            return carry

        lax.fori_loop(0, half, mate_slots, 0)
    g_copies += return_grads(1)

    for q in range(2):

        def own_comb(t, carry):
            grads = comb_grads(q, t, go[q * half + t])
            for p in range(2):
                gcf[q * half + t, piece(q, False, p)] = grads[p * quarter : (p + 1) * quarter]
            return carry

        lax.fori_loop(0, half, own_comb, 0)
    acc[...] = jnp.zeros_like(acc)
    arrive(c_copies)
    for q in range(2):

        def backward(t, carry):
            b = q * half + t
            for p in range(2):
                gcf[b, piece(q, True, p)] = gc_recv[q, t, p * quarter : (p + 1) * quarter].astype(F32)
            grad_comb = gcf[b]
            weights = comb[b]
            rowdot = jnp.sum(weights * grad_comb, axis=0, keepdims=True)
            wide = weights * (grad_comb - rowdot)
            gcf[b] = wide
            acc[...] += jnp.dot(wide.astype(BF), tok[b], preferred_element_type=F32)
            return carry

        lax.fori_loop(0, half, backward, 0)

    for k in range(1, m):
        there = flip(mz, k, m)
        psend[k] = acc[:, pl.ds(pl.multiple_of(there * cols, 128), cols)].astype(BF)
    z_copies = launch(to_dp(lambda k: psend.at[k], lambda k: precv.at[k], z_send, z_recv))

    def token_grads(b, carry):
        gt[b] = jnp.dot(gcf[b].T.astype(BF), allp[...], preferred_element_type=F32).astype(BF)
        return carry

    lax.fori_loop(0, imgs, token_grads, 0)
    put = pltpu.make_async_copy(gt, gt_out, local_sem.at[5])
    put.start()
    arrive(z_copies)
    total = acc[:, my_cols]
    for k in range(1, m):
        total = total + precv[k].astype(F32)
    acc[:, my_cols] = total
    for k in range(1, n):
        there = flip(me, k, n)
        xsend[k] = acc[pl.ds(pl.multiple_of(there * own, GROUP), own), my_cols].astype(BF)
    x_copies = launch([to_expert(xsend.at[k], xrecv.at[k], x_send.at[k], x_recv.at[k], k) for k in range(1, n)])
    arrive(x_copies)
    owned = acc[my_rows, my_cols]
    for k in range(1, n):
        owned = owned + xrecv[k].astype(F32)
    gp[...] = owned
    give = pltpu.make_async_copy(gp, gp_out, local_sem.at[6])
    give.start()

    arrive(g_copies)
    for copy in sent:
        copy.wait_send()
    for keep in keeps:
        keep.wait()
    put.wait()
    give.wait()


def paired_exchange(n, m, tok, go, so, par):
    imgs, patches, width = tok.shape
    own, all_img, _ = so.shape
    slots, cols, half = own * n, width // m, imgs // 2
    dma = pltpu.SemaphoreType.DMA
    return pl.pallas_call(
        functools.partial(paired_kernel, n, m),
        out_shape=(
            jax.ShapeDtypeStruct((n, imgs, own, width), BF),
            jax.ShapeDtypeStruct((imgs, patches, width), BF),
            jax.ShapeDtypeStruct((own, cols), F32),
        ),
        in_specs=[pl.BlockSpec(memory_space=pl.ANY)] * 4,
        out_specs=(pl.BlockSpec(memory_space=pl.ANY),) * 3,
        scratch_shapes=[
            pltpu.VMEM((imgs, patches, width), BF),
            pltpu.VMEM((imgs, patches, width), BF),
            pltpu.VMEM((2, half, patches, width), BF),
            pltpu.VMEM((own, all_img, width), BF),
            pltpu.VMEM((own, width), BF),
            pltpu.VMEM((slots, width), BF),
            pltpu.VMEM((2, 3, imgs, own, width), BF),
            pltpu.VMEM((2, 4, imgs, own, width), BF),
            pltpu.VMEM((2, 4, imgs, own, width), BF),
            pltpu.VMEM((imgs, slots, patches), F32),
            pltpu.VMEM((imgs, slots, patches), F32),
            pltpu.VMEM((2, imgs, slots // 2, patches), BF),
            pltpu.VMEM((2, half, slots // 2, patches), BF),
            pltpu.VMEM((2, half, slots // 2, patches), BF),
            pltpu.VMEM((2, half, slots // 2, patches), BF),
            pltpu.VMEM((imgs, patches, width), BF),
            pltpu.VMEM((slots, width), F32),
            pltpu.VMEM((m, slots, cols), BF),
            pltpu.VMEM((m, slots, cols), BF),
            pltpu.VMEM((n, own, cols), BF),
            pltpu.VMEM((n, own, cols), BF),
            pltpu.VMEM((own, cols), F32),
            dma((7,)), dma((2, 2)),
            dma((n,)), dma((n,)), dma((m,)), dma((m,)),
            dma((2,)), dma((2,)), dma((2, 3)), dma((2, 3)), dma((2,)), dma((2,)),
            dma((2,)), dma((2,)), dma((2, 2, 3)), dma((2, 2, 3)),
            dma((m,)), dma((m,)), dma((n,)), dma((n,)),
        ],
        compiler_params=pltpu.CompilerParams(
            collective_id=0, has_side_effects=True, vmem_limit_bytes=66 * 1000 * 1000
        ),
    )(tok, go, so, par)


def settle_kernel(arrived, gp_in, out, gp_out):
    all_img, group, width = arrived.shape
    span = GROUP * group
    row = lax.broadcasted_iota(jnp.int32, (span, span), 0)
    col = lax.broadcasted_iota(jnp.int32, (span, span), 1)
    pick = jnp.where(col == (row % GROUP) * group + row // GROUP, 1.0, 0.0).astype(BF)
    for at in range(0, all_img, GROUP):
        block = arrived[at : at + GROUP].reshape(span, width)
        moved = jnp.dot(pick, block, preferred_element_type=F32).astype(BF)
        out[:, at : at + GROUP, :] = moved.reshape(group, GROUP, width)
    gp_out[...] = gp_in[...]


def settle(arrived, grad_par):
    all_img, own, width = arrived.shape
    small = pl.BlockSpec((GROUP, grad_par.shape[1]), lambda i: (i, 0))
    return pl.pallas_call(
        settle_kernel,
        grid=(own // GROUP,),
        out_shape=(
            jax.ShapeDtypeStruct((own, all_img, width), BF),
            jax.ShapeDtypeStruct(grad_par.shape, F32),
        ),
        in_specs=[pl.BlockSpec((all_img, GROUP, width), lambda i: (0, i, 0)), small],
        out_specs=(pl.BlockSpec((GROUP, all_img, width), lambda i: (i, 0, 0)), small),
    )(arrived, grad_par)


def per_device(n, m, tokens, grad_out, slot_out, slot_params):
    tok = jnp.transpose(tokens, (1, 0, 2))
    go = jnp.transpose(grad_out, (1, 0, 2))
    plan = paired_exchange if n == 8 and tok.shape[0] % 2 == 0 else exchange
    arrived, grad_tok, grad_par = plan(n, m, tok, go, slot_out, slot_params)
    own, all_img, width = slot_out.shape
    grad_slot, grad_par = settle(arrived.reshape(all_img, own, width), grad_par)
    return jnp.transpose(grad_tok, (1, 0, 2)), grad_slot, grad_par


def solution(mesh):
    return jax.shard_map(
        functools.partial(per_device, mesh.shape["expert"], mesh.shape["dp"]),
        mesh=mesh,
        in_specs=(
            P(None, ("dp", "expert"), None),
            P(None, ("dp", "expert"), None),
            P("expert", "dp", None),
            P("expert", None),
        ),
        out_specs=(P(None, ("dp", "expert"), None), P("expert", "dp", None), P("expert", "dp")),
        check_vma=False,
    )
```

```python
import functools

import jax
import jax.numpy as jnp
from jax import lax
from jax.experimental import pallas as pl
from jax.experimental.pallas import tpu as pltpu
from jax.sharding import PartitionSpec as P

BF = jnp.bfloat16
F32 = jnp.float32
GROUP = 16


def flip(index, mask, size):
    total, bit = 0, 1
    while bit < size:
        total = total + ((index // bit + mask // bit) % 2) * bit
        bit *= 2
    return total


def send_order(n, core):
    if n != 8:
        return list(range(n - 1, 0, -1))
    masks = []
    for low in range(2):
        masks += [6 + low - 4 * core, 2 + low + 2 * core, 4 + low + 2 * core]
    return masks + [1]


def rows_last(lhs, rhs):
    return lax.dot_general(lhs, rhs, (((1,), (1,)), ((), ())), preferred_element_type=F32)


def exchange_kernel(
    n, m, tok_hbm, go_hbm, so_hbm, par_hbm,
    grec, gt_out, gp_out,
    tok, go, so, par, allp, stage, rows, gs, comb, gt, acc, psend, precv, xsend, xrecv, gp,
    local_sem, p_send, p_recv, q_send, q_recv, a_send, a_recv, g_send, g_recv,
    z_send, z_recv, x_send, x_recv,
):
    me = lax.axis_index("expert")
    mz = lax.axis_index("dp")
    core = me % 2
    imgs = tok.shape[0]
    own = par.shape[0]
    all_img = so.shape[1]
    cols = allp.shape[1] // m
    width = allp.shape[1]
    slots = allp.shape[0]
    my_cols = pl.ds(pl.multiple_of(mz * cols, 128), cols)
    my_rows = pl.ds(pl.multiple_of(me * own, GROUP), own)

    loads = [
        pltpu.make_async_copy(src, dst, local_sem.at[i])
        for i, (src, dst) in enumerate([(par_hbm, par), (so_hbm, so), (tok_hbm, tok), (go_hbm, go)])
    ]
    for load in loads:
        load.start()

    barrier = pltpu.get_barrier_semaphore()
    for k in range(1, n):
        pl.semaphore_signal(barrier, inc=1, device_id=(mz, flip(me, k, n)), device_id_type=pl.DeviceIdType.MESH)
    for k in range(1, m):
        pl.semaphore_signal(barrier, inc=1, device_id=(flip(mz, k, m), me), device_id_type=pl.DeviceIdType.MESH)
    pl.semaphore_wait(barrier, n + m - 2)

    def to_expert(src, dst, send, recv, k):
        return pltpu.make_async_remote_copy(
            src_ref=src, dst_ref=dst, send_sem=send.at[k], recv_sem=recv.at[k],
            device_id=(mz, flip(me, k, n)), device_id_type=pl.DeviceIdType.MESH,
        )

    def to_dp(src, dst, send, recv, k):
        return pltpu.make_async_remote_copy(
            src_ref=src, dst_ref=dst, send_sem=send.at[k], recv_sem=recv.at[k],
            device_id=(flip(mz, k, m), me), device_id_type=pl.DeviceIdType.MESH,
        )

    loads[0].wait()
    p_copies = [to_expert(par.at[:, my_cols], allp.at[my_rows, my_cols], p_send, p_recv, k) for k in range(1, n)]
    for copy in p_copies:
        copy.start()
    allp[my_rows, my_cols] = par[:, my_cols]

    loads[1].wait()
    out_r = lax.broadcasted_iota(jnp.int32, (imgs * GROUP, GROUP * all_img), 0)
    in_c = lax.broadcasted_iota(jnp.int32, (imgs * GROUP, GROUP * all_img), 1)
    base = in_c - (out_r % GROUP) * all_img - out_r // GROUP

    def relayout(dest, out):
        pick = jnp.where(base == dest * imgs, 1.0, 0.0).astype(BF)

        def one(g, carry):
            s0 = pl.multiple_of(g * GROUP, GROUP)
            block = so[pl.ds(s0, GROUP)].reshape(GROUP * all_img, width)
            moved = jnp.dot(pick, block, preferred_element_type=F32).astype(BF)
            out[:, pl.ds(s0, GROUP), :] = moved.reshape(imgs, GROUP, width)
            return carry

        lax.fori_loop(0, own // GROUP, one, 0)

    order = send_order(n, core)
    a_copies = []
    for k in order:
        relayout(flip(me, k, n), stage.at[k])
        copy = to_expert(stage.at[k], rows.at[me], a_send, a_recv, k)
        copy.start()
        a_copies.append(copy)
    relayout(me, rows.at[me])

    for copy in p_copies:
        copy.wait_recv()
    q_copies = [to_dp(allp.at[:, my_cols], allp.at[:, my_cols], q_send, q_recv, k) for k in range(1, m)]
    for copy in q_copies:
        copy.start()
    loads[2].wait()
    loads[3].wait()
    for copy in q_copies:
        copy.wait_recv()

    def forward(b, carry):
        logits = rows_last(allp[...], tok[b])
        peak = jnp.max(logits, axis=0, keepdims=True)
        raised = jnp.exp(logits - peak)
        weights = raised / jnp.sum(raised, axis=0, keepdims=True)
        comb[b] = weights
        grads = jnp.dot(weights.astype(BF), go[b], preferred_element_type=F32).astype(BF)
        gs[:, b] = grads.reshape(n, own, width)
        return carry

    lax.fori_loop(0, imgs, forward, 0)

    keep = pltpu.make_async_copy(gs.at[me], grec.at[me], local_sem.at[4])
    keep.start()
    g_copies = []
    for k in order:
        copy = to_expert(gs.at[flip(me, k, n)], grec.at[me], g_send, g_recv, k)
        copy.start()
        g_copies.append(copy)

    for copy in a_copies:
        copy.wait_recv()
    acc[...] = jnp.zeros_like(acc)

    def backward(b, carry):
        grad_comb = rows_last(rows[:, b].reshape(slots, width), go[b])
        weights = comb[b]
        rowdot = jnp.sum(weights * grad_comb, axis=0, keepdims=True)
        wide = weights * (grad_comb - rowdot)
        acc[...] += jnp.dot(wide.astype(BF), tok[b], preferred_element_type=F32)
        gt[b] = jnp.dot(wide.T.astype(BF), allp[...], preferred_element_type=F32).astype(BF)
        return carry

    lax.fori_loop(0, imgs, backward, 0)

    for k in range(1, m):
        there = flip(mz, k, m)
        psend[k] = acc[:, pl.ds(pl.multiple_of(there * cols, 128), cols)].astype(BF)
    z_copies = [to_dp(psend.at[k], precv.at[k], z_send, z_recv, k) for k in range(1, m)]
    for copy in z_copies:
        copy.start()
    put = pltpu.make_async_copy(gt, gt_out, local_sem.at[5])
    put.start()
    for copy in z_copies:
        copy.wait_recv()
    total = acc[:, my_cols]
    for k in range(1, m):
        total = total + precv[k].astype(F32)
    acc[:, my_cols] = total
    for k in range(1, n):
        there = flip(me, k, n)
        xsend[k] = acc[pl.ds(pl.multiple_of(there * own, GROUP), own), my_cols].astype(BF)
    x_copies = [to_expert(xsend.at[k], xrecv.at[k], x_send, x_recv, k) for k in range(1, n)]
    for copy in x_copies:
        copy.start()
    for copy in x_copies:
        copy.wait_recv()
    owned = acc[my_rows, my_cols]
    for k in range(1, n):
        owned = owned + xrecv[k].astype(F32)
    gp[...] = owned
    give = pltpu.make_async_copy(gp, gp_out, local_sem.at[6])
    give.start()

    for copy in g_copies:
        copy.wait_recv()
    for copy in p_copies + a_copies + q_copies + g_copies + z_copies + x_copies:
        copy.wait_send()
    keep.wait()
    put.wait()
    give.wait()


def exchange(n, m, tok, go, so, par):
    imgs, patches, width = tok.shape
    own, all_img, _ = so.shape
    slots, cols = own * n, width // m
    dma = pltpu.SemaphoreType.DMA
    return pl.pallas_call(
        functools.partial(exchange_kernel, n, m),
        out_shape=(
            jax.ShapeDtypeStruct((n, imgs, own, width), BF),
            jax.ShapeDtypeStruct((imgs, patches, width), BF),
            jax.ShapeDtypeStruct((own, cols), F32),
        ),
        in_specs=[pl.BlockSpec(memory_space=pl.ANY)] * 4,
        out_specs=(pl.BlockSpec(memory_space=pl.ANY),) * 3,
        scratch_shapes=[
            pltpu.VMEM((imgs, patches, width), BF),
            pltpu.VMEM((imgs, patches, width), BF),
            pltpu.VMEM((own, all_img, width), BF),
            pltpu.VMEM((own, width), BF),
            pltpu.VMEM((slots, width), BF),
            pltpu.VMEM((n, imgs, own, width), BF),
            pltpu.VMEM((n, imgs, own, width), BF),
            pltpu.VMEM((n, imgs, own, width), BF),
            pltpu.VMEM((imgs, slots, patches), F32),
            pltpu.VMEM((imgs, patches, width), BF),
            pltpu.VMEM((slots, width), F32),
            pltpu.VMEM((m, slots, cols), BF),
            pltpu.VMEM((m, slots, cols), BF),
            pltpu.VMEM((n, own, cols), BF),
            pltpu.VMEM((n, own, cols), BF),
            pltpu.VMEM((own, cols), F32),
            dma((7,)),
            dma((n,)), dma((n,)), dma((m,)), dma((m,)),
            dma((n,)), dma((n,)), dma((n,)), dma((n,)),
            dma((m,)), dma((m,)), dma((n,)), dma((n,)),
        ],
        compiler_params=pltpu.CompilerParams(
            collective_id=0, has_side_effects=True, vmem_limit_bytes=66 * 1000 * 1000
        ),
    )(tok, go, so, par)


AXES = ((2, (4, 5, 1)), (4, (2, 3, 1)))


def side_spot(which, index):
    high = index // 4 if which == 0 else (index // 2) % 2
    return high * 2 + index % 2


def paired_kernel(
    n, m, tok_hbm, go_hbm, so_hbm, par_hbm,
    grec, gt_out, gp_out,
    tok, go, mate, so, par, allp, stage, rows, gs, comb, gcf, low, low_send, gc_send, gc_recv,
    gt, acc, ksend, krecv, red, psend, precv, xsend, xrecv, gp,
    local_sem, keep_sem, p_send, p_recv, q_send, q_recv, f_send, f_recv, k_send, k_recv, o_send, o_recv, a_send, a_recv, w_send, w_recv,
    c_send, c_recv, g_send, g_recv, z_send, z_recv, x_send, x_recv,
):
    me = lax.axis_index("expert")
    mz = lax.axis_index("dp")
    imgs = tok.shape[0]
    half = imgs // 2
    own = par.shape[0]
    all_img = so.shape[1]
    slots, width = allp.shape
    patches = tok.shape[1]
    cols = width // m
    quarter = slots // 4
    my_cols = pl.ds(pl.multiple_of(mz * cols, 128), cols)
    my_rows = pl.ds(pl.multiple_of(me * own, GROUP), own)
    sides = ((me // 2) % 2, me // 4)

    def piece(which, other, p):
        side = 1 - sides[which] if other else sides[which]
        start = p * 2 * quarter + side * quarter if which == 0 else side * 2 * quarter + p * quarter
        return pl.ds(pl.multiple_of(start, quarter), quarter)

    loads = [
        pltpu.make_async_copy(src, dst, local_sem.at[i])
        for i, (src, dst) in enumerate([(par_hbm, par), (so_hbm, so), (tok_hbm, tok), (go_hbm, go)])
    ]
    for i in (0, 3, 1, 2):
        loads[i].start()

    barrier = pltpu.get_barrier_semaphore()
    for k in range(1, n):
        pl.semaphore_signal(barrier, inc=1, device_id=(mz, flip(me, k, n)), device_id_type=pl.DeviceIdType.MESH)
    for k in range(1, m):
        pl.semaphore_signal(barrier, inc=1, device_id=(flip(mz, k, m), me), device_id_type=pl.DeviceIdType.MESH)
    pl.semaphore_wait(barrier, n + m - 2)

    def to_expert(src, dst, send, recv, k):
        return pltpu.make_async_remote_copy(
            src_ref=src, dst_ref=dst, send_sem=send, recv_sem=recv,
            device_id=(mz, flip(me, k, n)), device_id_type=pl.DeviceIdType.MESH,
        )

    def to_dp(src, dst, send, recv):
        return [
            pltpu.make_async_remote_copy(
                src_ref=src(k), dst_ref=dst(k), send_sem=send.at[k], recv_sem=recv.at[k],
                device_id=(flip(mz, k, m), me), device_id_type=pl.DeviceIdType.MESH,
            )
            for k in range(1, m)
        ]

    sent = []

    def launch(copies):
        for copy in copies:
            copy.start()
        sent.extend(copies)
        return copies

    def arrive(copies):
        for copy in copies:
            copy.wait_recv()

    loads[0].wait()
    p_copies = launch([
        to_expert(par.at[:, my_cols], allp.at[my_rows, my_cols], p_send.at[k], p_recv.at[k], k)
        for k in range(2, n, 2)
    ])
    allp[my_rows, my_cols] = par[:, my_cols]
    loads[3].wait()
    o_copies = launch([
        to_expert(go.at[pl.ds(q * half, half)], mate.at[q], o_send.at[q], o_recv.at[q], AXES[q][0]) for q in range(2)
    ])

    loads[1].wait()
    out_r = lax.broadcasted_iota(jnp.int32, (imgs * GROUP, GROUP * all_img), 0)
    in_c = lax.broadcasted_iota(jnp.int32, (imgs * GROUP, GROUP * all_img), 1)
    base = in_c - (out_r % GROUP) * all_img - (out_r // GROUP) % half
    first = out_r < half * GROUP

    def relayout(q, dest, out):
        own_at = dest * imgs + q * half
        mate_at = flip(dest, AXES[q][0], n) * imgs + q * half
        pick = jnp.where(base == jnp.where(first, own_at, mate_at), 1.0, 0.0).astype(BF)

        def one(g, carry):
            s0 = pl.multiple_of(g * GROUP, GROUP)
            block = so[pl.ds(s0, GROUP)].reshape(GROUP * all_img, width)
            moved = jnp.dot(pick, block, preferred_element_type=F32).astype(BF)
            out[:, pl.ds(s0, GROUP), :] = moved.reshape(imgs, GROUP, width)
            return carry

        lax.fori_loop(0, own // GROUP, one, 0)

    a_copies = []
    for i in range(3):
        for q in range(2):
            k = AXES[q][1][i]
            relayout(q, flip(me, k, n), stage.at[q, i])
            a_copies += launch([
                to_expert(stage.at[q, i], rows.at[q, side_spot(q, me)], a_send.at[q, i], a_recv.at[q, i], k)
            ])
    for q in range(2):
        relayout(q, me, rows.at[q, side_spot(q, me)])

    arrive(p_copies)
    q_copies = []
    for i in range(n // 2):
        block = allp.at[pl.ds(pl.multiple_of(flip(me, 2 * i, n) * own, GROUP), own), my_cols]
        q_copies += launch(to_dp(lambda k: block, lambda k: block, q_send.at[i], q_recv.at[i]))
    loads[2].wait()
    arrive(q_copies)
    f_copies = []
    for i in range(n // 2):
        block = allp.at[pl.ds(pl.multiple_of(flip(me, 2 * i, n) * own, GROUP), own)]
        f_copies += launch([to_expert(block, block, f_send.at[i], f_recv.at[i], 1)])
    arrive(f_copies)

    w_copies = []
    for q in range(2):

        def forward(t, carry):
            b = q * half + t
            logits = rows_last(allp[...], tok[b])
            peak = jnp.max(logits, axis=0, keepdims=True)
            raised = jnp.exp(logits - peak)
            comb[b] = raised / jnp.sum(raised, axis=0, keepdims=True)
            for p in range(2):
                low[q, t, p * quarter : (p + 1) * quarter] = comb[b, piece(q, False, p)].astype(BF)
                low_send[q, t, p * quarter : (p + 1) * quarter] = comb[b, piece(q, True, p)].astype(BF)
            return carry

        lax.fori_loop(0, half, forward, 0)
        w_copies += launch([
            to_expert(low_send.at[q], low.at[q, pl.ds(half, half)], w_send.at[q], w_recv.at[q], AXES[q][0])
        ])

    def slot_grads(q, i, grads_in):
        out = jnp.dot(low[q, i], grads_in, preferred_element_type=F32).astype(BF)
        gs[q, :, i] = out.reshape(4, own, width)

    def comb_grads(q, i, grads_in):
        return rows_last(rows[q, :, i].reshape(4 * own, width), grads_in)

    for q in range(2):

        def own_slots(t, carry):
            slot_grads(q, t, go[q * half + t])
            return carry

        lax.fori_loop(0, half, own_slots, 0)

    arrive(o_copies)
    arrive(a_copies)
    c_copies = []
    for q in range(2):

        def mate_comb(t, carry):
            gc_send[q, t] = comb_grads(q, half + t, mate[q, t]).astype(BF)
            return carry

        lax.fori_loop(0, half, mate_comb, 0)
        c_copies += launch([to_expert(gc_send.at[q], gc_recv.at[q], c_send.at[q], c_recv.at[q], AXES[q][0])])

    keeps = []

    def return_grads(h):
        copies = []
        for i in range(3):
            for q in range(2):
                k = AXES[q][1][i]
                holder = flip(me, AXES[q][0], n) if h else me
                part, images = pl.ds(h * half, half), pl.ds(q * half, half)
                copies += launch([
                    to_expert(
                        gs.at[q, side_spot(q, flip(me, k, n)), part], grec.at[holder, images],
                        g_send.at[h, q, i], g_recv.at[h, q, i], k,
                    )
                ])
        for q in range(2):
            holder = flip(me, AXES[q][0], n) if h else me
            keep = pltpu.make_async_copy(
                gs.at[q, side_spot(q, me), pl.ds(h * half, half)],
                grec.at[holder, pl.ds(q * half, half)], keep_sem.at[h, q],
            )
            keep.start()
            keeps.append(keep)
        return copies

    g_copies = return_grads(0)
    arrive(w_copies)
    for q in range(2):

        def mate_slots(t, carry):
            slot_grads(q, half + t, mate[q, t])
            return carry

        lax.fori_loop(0, half, mate_slots, 0)
    g_copies += return_grads(1)

    for q in range(2):

        def own_comb(t, carry):
            grads = comb_grads(q, t, go[q * half + t])
            for p in range(2):
                gcf[q * half + t, piece(q, False, p)] = grads[p * quarter : (p + 1) * quarter]
            return carry

        lax.fori_loop(0, half, own_comb, 0)
    acc[...] = jnp.zeros_like(acc)
    arrive(c_copies)
    for q in range(2):

        def backward(t, carry):
            b = q * half + t
            for p in range(2):
                gcf[b, piece(q, True, p)] = gc_recv[q, t, p * quarter : (p + 1) * quarter].astype(F32)
            grad_comb = gcf[b]
            weights = comb[b]
            rowdot = jnp.sum(weights * grad_comb, axis=0, keepdims=True)
            wide = weights * (grad_comb - rowdot)
            gcf[b] = wide
            acc[...] += jnp.dot(wide.astype(BF), tok[b], preferred_element_type=F32)
            return carry

        lax.fori_loop(0, half, backward, 0)

    core = me % 2
    for i in range(n // 2):
        ksend[i] = acc[pl.ds(pl.multiple_of((2 * i + 1 - core) * own, GROUP), own)].astype(BF)
    k_copies = launch([to_expert(ksend, krecv, k_send.at[0], k_recv.at[0], 1)])
    arrive(k_copies)
    for i in range(n // 2):
        red[i] = acc[pl.ds(pl.multiple_of((2 * i + core) * own, GROUP), own)] + krecv[i].astype(F32)
    for k in range(1, m):
        there = flip(mz, k, m)
        psend[k] = red[:, :, pl.ds(pl.multiple_of(there * cols, 128), cols)].astype(BF)
    z_copies = launch(to_dp(lambda k: psend.at[k], lambda k: precv.at[k], z_send, z_recv))

    def token_grads(b, carry):
        gt[b] = jnp.dot(gcf[b].T.astype(BF), allp[...], preferred_element_type=F32).astype(BF)
        return carry

    lax.fori_loop(0, imgs, token_grads, 0)
    put = pltpu.make_async_copy(gt, gt_out, local_sem.at[5])
    put.start()
    arrive(z_copies)
    total = red[:, :, my_cols]
    for k in range(1, m):
        total = total + precv[k].astype(F32)
    red[:, :, my_cols] = total
    for k in range(2, n, 2):
        xsend[k // 2] = red[flip(me, k, n) // 2, :, my_cols].astype(BF)
    x_copies = launch([
        to_expert(xsend.at[k // 2], xrecv.at[k // 2], x_send.at[k], x_recv.at[k], k) for k in range(2, n, 2)
    ])
    arrive(x_copies)
    owned = red[me // 2, :, my_cols]
    for k in range(2, n, 2):
        owned = owned + xrecv[k // 2].astype(F32)
    gp[...] = owned
    give = pltpu.make_async_copy(gp, gp_out, local_sem.at[6])
    give.start()

    arrive(g_copies)
    for copy in sent:
        copy.wait_send()
    for keep in keeps:
        keep.wait()
    put.wait()
    give.wait()


def paired_exchange(n, m, tok, go, so, par):
    imgs, patches, width = tok.shape
    own, all_img, _ = so.shape
    slots, cols, half = own * n, width // m, imgs // 2
    dma = pltpu.SemaphoreType.DMA
    return pl.pallas_call(
        functools.partial(paired_kernel, n, m),
        out_shape=(
            jax.ShapeDtypeStruct((n, imgs, own, width), BF),
            jax.ShapeDtypeStruct((imgs, patches, width), BF),
            jax.ShapeDtypeStruct((own, cols), F32),
        ),
        in_specs=[pl.BlockSpec(memory_space=pl.ANY)] * 4,
        out_specs=(pl.BlockSpec(memory_space=pl.ANY),) * 3,
        scratch_shapes=[
            pltpu.VMEM((imgs, patches, width), BF),
            pltpu.VMEM((imgs, patches, width), BF),
            pltpu.VMEM((2, half, patches, width), BF),
            pltpu.VMEM((own, all_img, width), BF),
            pltpu.VMEM((own, width), BF),
            pltpu.VMEM((slots, width), BF),
            pltpu.VMEM((2, 3, imgs, own, width), BF),
            pltpu.VMEM((2, 4, imgs, own, width), BF),
            pltpu.VMEM((2, 4, imgs, own, width), BF),
            pltpu.VMEM((imgs, slots, patches), F32),
            pltpu.VMEM((imgs, slots, patches), F32),
            pltpu.VMEM((2, imgs, slots // 2, patches), BF),
            pltpu.VMEM((2, half, slots // 2, patches), BF),
            pltpu.VMEM((2, half, slots // 2, patches), BF),
            pltpu.VMEM((2, half, slots // 2, patches), BF),
            pltpu.VMEM((imgs, patches, width), BF),
            pltpu.VMEM((slots, width), F32),
            pltpu.VMEM((n // 2, own, width), BF),
            pltpu.VMEM((n // 2, own, width), BF),
            pltpu.VMEM((n // 2, own, width), F32),
            pltpu.VMEM((m, n // 2, own, cols), BF),
            pltpu.VMEM((m, n // 2, own, cols), BF),
            pltpu.VMEM((n // 2, own, cols), BF),
            pltpu.VMEM((n // 2, own, cols), BF),
            pltpu.VMEM((own, cols), F32),
            dma((7,)), dma((2, 2)),
            dma((n,)), dma((n,)), dma((n // 2, m)), dma((n // 2, m)),
            dma((n // 2,)), dma((n // 2,)), dma((1,)), dma((1,)),
            dma((2,)), dma((2,)), dma((2, 3)), dma((2, 3)), dma((2,)), dma((2,)),
            dma((2,)), dma((2,)), dma((2, 2, 3)), dma((2, 2, 3)),
            dma((m,)), dma((m,)), dma((n,)), dma((n,)),
        ],
        compiler_params=pltpu.CompilerParams(
            collective_id=0, has_side_effects=True, vmem_limit_bytes=66 * 1000 * 1000
        ),
    )(tok, go, so, par)


def settle_kernel(arrived, gp_in, out, gp_out):
    out[...] = jnp.swapaxes(arrived[...], 0, 1)
    gp_out[...] = gp_in[...]


def settle(arrived, grad_par):
    all_img, own, width = arrived.shape
    small = pl.BlockSpec((GROUP, grad_par.shape[1]), lambda i: (i, 0))
    return pl.pallas_call(
        settle_kernel,
        grid=(own // GROUP,),
        out_shape=(
            jax.ShapeDtypeStruct((own, all_img, width), BF),
            jax.ShapeDtypeStruct(grad_par.shape, F32),
        ),
        in_specs=[pl.BlockSpec((all_img, GROUP, width), lambda i: (0, i, 0)), small],
        out_specs=(pl.BlockSpec((GROUP, all_img, width), lambda i: (i, 0, 0)), small),
    )(arrived, grad_par)


def per_device(n, m, tokens, grad_out, slot_out, slot_params):
    tok = jnp.transpose(tokens, (1, 0, 2))
    go = jnp.transpose(grad_out, (1, 0, 2))
    plan = paired_exchange if n == 8 and tok.shape[0] % 2 == 0 else exchange
    arrived, grad_tok, grad_par = plan(n, m, tok, go, slot_out, slot_params)
    own, all_img, width = slot_out.shape
    grad_slot, grad_par = settle(arrived.reshape(all_img, own, width), grad_par)
    return jnp.transpose(grad_tok, (1, 0, 2)), grad_slot, grad_par


def solution(mesh):
    return jax.shard_map(
        functools.partial(per_device, mesh.shape["expert"], mesh.shape["dp"]),
        mesh=mesh,
        in_specs=(
            P(None, ("dp", "expert"), None),
            P(None, ("dp", "expert"), None),
            P("expert", "dp", None),
            P("expert", None),
        ),
        out_specs=(P(None, ("dp", "expert"), None), P("expert", "dp", None), P("expert", "dp")),
        check_vma=False,
    )
```
